32 devices in a mesh: dp: 4 (over z), mp: 8 (over y, x, core).
Axes of the slice: x: 2, y: 2, z: 4, core: 2. Of those that a mesh axis runs over, the one named last changes fastest.
Arguments:
- inputs: bfloat16 [197, 49152], P(None, ('dp', 'mp')), may hold values from -6 to 6
- cotangent: bfloat16 [197, 49152], P(None, ('dp', 'mp')), may hold values from -1.1953125 to 1.1953125
- w_in: bfloat16 [768, 3072], P('dp', 'mp'), may hold values from -0.21875 to 0.21875
- w_out: bfloat16 [3072, 768], P('mp', 'dp'), may hold values from -0.109375 to 0.109375
- prec_in: float32 [768, 3072], P('dp', 'mp'), may hold values from 0.1 to 2
- prec_out: float32 [3072, 768], P('mp', 'dp'), may hold values from 0.1 to 2
Outputs:
- new_prec_in: float32 [768, 3072], P('dp', 'mp')
- new_prec_out: float32 [3072, 768], P('mp', 'dp')
- new_w_in: float32 [768, 3072], P('dp', 'mp')
- new_w_out: float32 [3072, 768], P('mp', 'dp')
The draws below stay inside these ranges and needn't reach their ends.
All inputs are finite; a program needn't handle non-finite values.
Results may differ from the reference program's by a relative error of at most 0.0028.
Values may be sent and summed in bfloat16 or wider, within the bound.
A program may use at most 64 MiB of HBM per device.

```python
import math
import jax
import jax.numpy as jnp
from jax import lax

D = 768
HID = 3072
SEQ = 197
IMAGES = 64


def shard_levels(own_key, extent, cuts, least, high):
    factor_of = 1.0
    for axis_at, parts in cuts:
        heights = jax.random.uniform(jax.random.fold_in(jax.random.fold_in(own_key, 6), axis_at), (parts,), jnp.float32, least / len(cuts), high / len(cuts))
        factor_of = factor_of * jnp.repeat(jnp.exp(heights), extent[axis_at] // parts).reshape((-1,) + (1,) * (len(extent) - 1 - axis_at))
    return factor_of


def centred(rng, extent, deviation, bound, shards=(), held_as=jnp.bfloat16):
    values = deviation * jax.random.normal(rng, extent, jnp.float32)
    if shards:
        values = values * shard_levels(rng, extent, shards, -0.22, 0.18)
    return jnp.clip(values, -bound, bound).astype(held_as)


def setup_inputs(seed: int = 0) -> dict:
    key_of = jax.random.split(jax.random.key(seed), 7)
    return {
        "inputs": centred(key_of[0], (SEQ, IMAGES * D), 1.0, 6.0, ((1, 32),)),
        "cotangent": centred(key_of[1], (SEQ, IMAGES * D), 0.2, 1.1953125, ((1, 32),)),
        "w_in": centred(key_of[2], (D, HID), D ** -0.5, 0.21875, ((0, 4), (1, 8))),
        "w_out": centred(key_of[3], (HID, D), HID ** -0.5, 0.109375, ((0, 8), (1, 4))),
        "prec_in": jnp.clip(jnp.exp(math.log(2.0) - 2.9957323 * jax.random.uniform(key_of[4], (D, HID), jnp.float32) ** shard_levels(key_of[4], (D, HID), ((0, 4), (1, 8)), -0.2, 0.2)), 0.1, 2.0),
        "prec_out": jnp.clip(jnp.exp(math.log(2.0) - 2.9957323 * jax.random.uniform(key_of[5], (HID, D), jnp.float32) ** shard_levels(key_of[5], (HID, D), ((0, 8), (1, 4)), -0.2, 0.2)), 0.1, 2.0),
    }


def gelu_tanh(v):
    return jax.nn.gelu(v, approximate=True)

def reference(inputs, cotangent, w_in, w_out, prec_in, prec_out):
    images = inputs.shape[1] // D
    inputs3 = jnp.transpose(inputs.reshape(SEQ, images, D), (1, 0, 2))
    cot3 = jnp.transpose(cotangent.reshape(SEQ, images, D), (1, 0, 2))

    def one_image(carry, item):
        sum_in, sq_in, sum_out, sq_out = carry
        rows, grads = item
        pre = jnp.dot(rows, w_in, preferred_element_type=jnp.float32)
        act = gelu_tanh(pre).astype(jnp.bfloat16)
        back = jnp.dot(grads, w_out.T, preferred_element_type=jnp.float32)
        delta = jax.vjp(gelu_tanh, pre)[1](back)[0].astype(jnp.bfloat16)
        g_in = jnp.dot(rows.T, delta, preferred_element_type=jnp.float32)
        g_out = jnp.dot(act.T, grads, preferred_element_type=jnp.float32)
        return ((sum_in + g_in, sq_in + g_in * g_in, sum_out + g_out, sq_out + g_out * g_out), None)
    zeros_in = jnp.zeros((D, HID), jnp.float32)
    zeros_out = jnp.zeros((HID, D), jnp.float32)
    totals, _ = lax.scan(one_image, (zeros_in, zeros_in, zeros_out, zeros_out), (inputs3, cot3))
    sum_in, sq_in, sum_out, sq_out = totals
    scale = 1.0 / images
    new_prec_in = 0.6 * prec_in + 0.4 * sq_in * scale
    new_prec_out = 0.6 * prec_out + 0.4 * sq_out * scale
    win = w_in.astype(jnp.float32)
    wout = w_out.astype(jnp.float32)
    new_w_in = win - 1.0 * (sum_in * scale + 0.1 * win) / (new_prec_in + 0.1)
    new_w_out = wout - 1.0 * (sum_out * scale + 0.1 * wout) / (new_prec_out + 0.1)
    return (new_prec_in, new_prec_out, new_w_in, new_w_out)
```

```python
import functools
import jax
import jax.numpy as jnp
from jax import lax
from jax.experimental import pallas as pl
from jax.experimental.pallas import tpu as pltpu
from jax.sharding import PartitionSpec as P


def gelu_tanh(v):
    return jax.nn.gelu(v, approximate=True)


def per_device(inputs, cotangent, w_in, w_out, prec_in, prec_out):
    SEQ = inputs.shape[0]
    D = w_in.shape[0] * lax.axis_size("dp")
    w_in_full, w_out_full = (
        lax.all_gather(w_in, "dp", axis=0, tiled=True),
        lax.all_gather(w_out, "dp", axis=1, tiled=True),
    )
    whole = lax.all_gather(inputs, "mp", axis=1, tiled=True)
    rows3 = whole.reshape(SEQ, -1, D)
    images = rows3.shape[1]
    pre = jnp.einsum("snd,dh->snh", rows3, w_in_full, preferred_element_type=jnp.float32)
    act = gelu_tanh(pre).astype(jnp.bfloat16)
    cot_whole = lax.all_gather(cotangent, "mp", axis=1, tiled=True)
    cot3 = cot_whole.reshape(SEQ, images, D)
    back = jnp.einsum("snd,hd->snh", cot3, w_out_full, preferred_element_type=jnp.float32)
    per_out = jnp.einsum("snh,snd->nhd", act, cot3, preferred_element_type=jnp.float32)
    sum_out = jnp.sum(per_out, 0)
    sq_out = jnp.sum(per_out * per_out, 0)
    delta = jax.vjp(gelu_tanh, pre)[1](back)[0].astype(jnp.bfloat16)
    rows_again = lax.all_gather(inputs, "mp", axis=1, tiled=True).reshape(SEQ, images, D)
    per_in = jnp.einsum("snd,snh->ndh", rows_again, delta, preferred_element_type=jnp.float32)
    sum_in = jnp.sum(per_in, 0)
    sq_in = jnp.sum(per_in * per_in, 0)
    sum_in, sq_in = (
        lax.psum_scatter(sum_in, "dp", scatter_dimension=0, tiled=True),
        lax.psum_scatter(sq_in, "dp", scatter_dimension=0, tiled=True),
    )
    sum_out, sq_out = (
        lax.psum_scatter(sum_out, "dp", scatter_dimension=1, tiled=True),
        lax.psum_scatter(sq_out, "dp", scatter_dimension=1, tiled=True),
    )
    scale = 1.0 / (images * lax.axis_size("dp"))
    new_prec_in = 0.6 * prec_in + 0.4 * sq_in * scale
    new_prec_out = 0.6 * prec_out + 0.4 * sq_out * scale
    w_in_own = w_in.astype(jnp.float32)
    w_out_own = w_out.astype(jnp.float32)
    new_w_in = w_in_own - 1.0 * (sum_in * scale + 0.1 * w_in_own) / (new_prec_in + 0.1)
    new_w_out = w_out_own - 1.0 * (sum_out * scale + 0.1 * w_out_own) / (new_prec_out + 0.1)
    return (new_prec_in, new_prec_out, new_w_in, new_w_out)


F32, BF16 = jnp.float32, jnp.bfloat16
NT = (((1,), (1,)), ((), ()))
MESH = pl.DeviceIdType.MESH


def dot(a, b):
    return jnp.dot(a, b, preferred_element_type=F32)


def dot_nt(a, b):
    return lax.dot_general(a, b, NT, preferred_element_type=F32)


def kernel(
    x_hbm, c_hbm, win_ref, wout_t_ref, wout_ref, pin_ref, pout_ref,
    o_pin, o_pout, o_win, o_wout,
    xg, cg, wg_in, wg_out, w_in_t, w_out_f, act, slope, back, delta,
    acc, own, stage, recv,
    loc, ici_s, ici_r, d2d_s, d2d_r, w_s, w_r, rs_s, rs_r,
):
    z, m = lax.axis_index("dp"), lax.axis_index("mp")
    core, q = lax.rem(m, 2), m // 2
    xx, yy = lax.rem(q, 2), q // 2
    chips = [yy * 2 + xx, yy * 2 + 1 - xx, (1 - yy) * 2 + xx, (1 - yy) * 2 + 1 - xx]
    same = [2 * chip + core for chip in chips]
    other = [2 * chip + 1 - core for chip in chips]
    xn, yn, partner_id = same[1], same[2], other[0]
    depth = win_ref.shape[0]
    width = 4 * depth
    lo = -(-depth // 128) * 128
    hi = 3 * depth // 128 * 128
    ranges = ((0, lo), (hi, width), (lo, hi))
    images = xg.shape[0]

    def view(p, mm):
        if p < 2:
            return xg.at[2 * mm + p]
        left, right = ranges[(p - 2) // 2]
        return cg.at[2 * mm + (p - 2) % 2, :, pl.ds(left, right - left)]

    def remote(p, mm, to, ssem, rsem):
        return pltpu.make_async_remote_copy(
            src_ref=view(p, mm), dst_ref=view(p, mm), send_sem=ssem, recv_sem=rsem,
            device_id=(z, to), device_id_type=MESH,
        )

    def to_x(p):
        return remote(p, m, xn, ici_s.at[p, 0], ici_r.at[p, 0])

    def to_y(p):
        return remote(p, m, yn, ici_s.at[p, 1], ici_r.at[p, 1])

    def relayed(p):
        first = p % 2 == 0
        return remote(p, same[1 if first else 2], yn if first else xn, ici_s.at[p, 2], ici_r.at[p, 2])

    def across(p, s):
        return remote(p, same[s], partner_id, d2d_s.at[p, s], d2d_r.at[p, s])

    def arrived(p, s):
        remote(p, same[s], xn, ici_s.at[p, 0], ici_r.at[p, s - 1]).wait_recv()

    def from_partner(pieces, s):
        for p in pieces:
            remote(p, other[s], partner_id, d2d_s.at[p, s], d2d_r.at[p, s]).wait_recv()

    def own_sends(even, odd):
        for a, b in ((even, odd),):
            for p in a:
                to_x(p).start()
            for p in b:
                to_y(p).start()
            for p in b:
                to_x(p).start()
            for p in a:
                to_y(p).start()

    def relay(even, odd):
        for p in even:
            arrived(p, 1)
            relayed(p).start()
        for p in odd:
            arrived(p, 2)
            relayed(p).start()
        for p in even:
            across(p, 1).start()
        for p in odd:
            across(p, 2).start()

    def second(even, odd):
        for p in odd:
            arrived(p, 1)
            across(p, 1).start()
        for p in even:
            arrived(p, 2)
            across(p, 2).start()

    def third(even, odd):
        for p in even + odd:
            arrived(p, 3)
            across(p, 3).start()

    x_even, x_odd = [0], [1]
    a_even, a_odd = [2, 4], [3, 5]
    b_even, b_odd = [6], [7]

    locals_ = []
    for i in range(2):
        cols = pl.ds(i * width, width)
        locals_.append(pltpu.make_async_copy(x_hbm.at[:, cols], xg.at[2 * m + i], loc.at[i]))
    for i in range(2):
        cols = pl.ds(i * width, width)
        locals_.append(pltpu.make_async_copy(c_hbm.at[:, cols], cg.at[2 * m + i], loc.at[2 + i]))
    for copy in locals_:
        copy.start()

    barrier = pltpu.get_barrier_semaphore()
    zs = [lax.rem(z + o, 4) for o in (1, 2, 3)]
    peers = [(z, xn), (z, yn), (z, partner_id)] + [(there, m) for there in zs]
    for peer in peers:
        pl.semaphore_signal(barrier, inc=1, device_id=peer, device_id_type=MESH)
    pl.semaphore_wait(barrier, len(peers))

    locals_[0].wait()
    locals_[1].wait()
    own_sends(x_even, x_odd)
    for p in x_even + x_odd:
        across(p, 0).start()

    rows = pl.ds(pl.multiple_of(z * depth, 16), depth)

    def weight(k, o):
        src, dst = ((win_ref, wg_in), (wout_t_ref, wg_out))[k]
        return pltpu.make_async_remote_copy(
            src_ref=src, dst_ref=dst.at[rows], send_sem=w_s.at[k, o], recv_sem=w_r.at[k, o],
            device_id=(zs[o], m), device_id_type=MESH,
        )

    for k in range(2):
        for o in range(3):
            weight(k, o).start()
    locals_[2].wait()
    locals_[3].wait()
    for p in a_even + a_odd + b_even + b_odd:
        across(p, 0).start()
    wg_in[rows, :] = win_ref[...]
    wg_out[rows, :] = wout_t_ref[...]
    acc[...] = jnp.zeros_like(acc)

    def forward(chip):
        def one(j, carry):
            n = 4 * chip + j
            pre = dot_nt(w_in_t[...], xg[n])
            square = pre * pre
            t = jnp.tanh(0.7978845608028654 * pre * (1.0 + 0.044715 * square))
            half = 0.5 * (1.0 + t)
            act[n] = (pre * half).astype(BF16)
            slope[n] = half + 0.5 * pre * (1.0 - t * t) * (0.7978845608028654 * (1.0 + 0.134145 * square))
            return carry
        lax.fori_loop(0, 4, one, 0)

    def accumulate(lhs, rhs, first, count, span):
        cols = slice(*span)
        gs = [dot(lhs[first + j], rhs[first + j, :, cols]) for j in range(count)]
        total, squares = gs[0], gs[0] * gs[0]
        for g in gs[1:]:
            total, squares = total + g, squares + g * g
        acc[0, :, cols] += total
        acc[1, :, cols] += squares

    def chunk_a(chip):
        def pair(h, carry):
            first = 4 * chip + 2 * h
            for j in range(2):
                n = first + j
                back[n] = dot_nt(w_out_f[:, 0:lo], cg[n, :, 0:lo]) + dot_nt(w_out_f[:, hi:width], cg[n, :, hi:width])
            for span in ranges[:2]:
                accumulate(act, cg, first, 2, span)
            return carry
        lax.fori_loop(0, 2, pair, 0)

    def chunk_b(chip):
        def pair(h, carry):
            first = 4 * chip + 2 * h
            for j in range(2):
                n = first + j
                whole = back[n] + dot_nt(w_out_f[:, lo:hi], cg[n, :, lo:hi])
                delta[n] = (whole * slope[n]).astype(BF16)
            accumulate(act, cg, first, 2, ranges[2])
            return carry
        lax.fori_loop(0, 2, pair, 0)

    def settle(part, span):
        cols = slice(*span)
        for a in range(2):
            turned = acc[a, :, cols].T
            own[part, a, cols, :] = turned
            stage[part, a, cols, :] = turned.astype(BF16)
            if part == 0:
                acc[a, :, cols] = jnp.zeros_like(acc[a, :, cols])

    def reduce_copy(part, j):
        slot = lax.rem(z - j + 3, 4)
        return pltpu.make_async_remote_copy(
            src_ref=stage.at[part, :, pl.ds(j * depth, depth), :], dst_ref=recv.at[part, slot],
            send_sem=rs_s.at[part, j], recv_sem=rs_r.at[part, slot],
            device_id=(j, m), device_id_type=MESH,
        )

    def give(part, targets):
        for j in targets:
            @pl.when(z != j)
            def _():
                reduce_copy(part, j).start()

    relay(x_even, x_odd)
    own_sends(a_even, a_odd)
    for o in range(3):
        weight(0, o).wait_recv()
    w_in_t[...] = wg_in[...].astype(F32).T.astype(BF16)
    from_partner([0, 1], 0)
    forward(chips[0])
    second(x_even, x_odd)
    from_partner([0, 1], 1)
    forward(chips[1])
    from_partner([0, 1], 2)
    forward(chips[2])
    third(x_even, x_odd)
    from_partner([0, 1], 3)
    forward(chips[3])

    for o in range(3):
        weight(1, o).wait_recv()
    w_out_f[...] = wg_out[...].astype(F32).T.astype(BF16)
    pieces = a_even + a_odd
    relay(a_even, a_odd)
    own_sends(b_even, b_odd)
    from_partner(pieces, 0)
    chunk_a(chips[0])
    second(a_even, a_odd)
    from_partner(pieces, 1)
    chunk_a(chips[1])
    from_partner(pieces, 2)
    chunk_a(chips[2])
    third(a_even, a_odd)
    relay(b_even, b_odd)
    from_partner(pieces, 3)
    chunk_a(chips[3])
    settle(0, ranges[0])
    give(0, [0])
    settle(0, ranges[1])
    give(0, [3])

    pieces = b_even + b_odd
    from_partner(pieces, 0)
    chunk_b(chips[0])
    second(b_even, b_odd)
    from_partner(pieces, 1)
    chunk_b(chips[1])
    from_partner(pieces, 2)
    chunk_b(chips[2])
    third(b_even, b_odd)
    from_partner(pieces, 3)
    chunk_b(chips[3])
    settle(0, ranges[2])
    give(0, [1, 2])

    for span, targets in zip(ranges, ([0], [3], [1, 2])):
        def four(k, carry, span=span):
            accumulate(delta, xg, 4 * k, 4, span)
            return carry
        lax.fori_loop(0, images // 4, four, 0)
        settle(1, span)
        give(1, targets)

    scale = 1.0 / (images * 4)

    def collected(part):
        for t in range(3):
            pltpu.make_async_remote_copy(
                src_ref=stage.at[part, :, pl.ds(0, depth), :], dst_ref=recv.at[part, t],
                send_sem=rs_s.at[part, 0], recv_sem=rs_r.at[part, t],
                device_id=(zs[t], m), device_id_type=MESH,
            ).wait_recv()
        found = []
        for a in range(2):
            total = own[part, a, rows, :]
            for t in range(3):
                total = total + recv[part, t, a].astype(F32)
            found.append(total)
        return found

    total, squares = collected(0)
    prec = 0.6 * pout_ref[...] + 0.4 * squares.T * scale
    o_pout[...] = prec
    mean = wout_ref[...].astype(F32)
    o_wout[...] = mean - (total.T * scale + 0.1 * mean) / (prec + 0.1)
    total, squares = collected(1)
    prec = 0.6 * pin_ref[...] + 0.4 * squares * scale
    o_pin[...] = prec
    mean = win_ref[...].astype(F32)
    o_win[...] = mean - (total * scale + 0.1 * mean) / (prec + 0.1)

    for p in range(8):
        to_x(p).wait_send()
        to_y(p).wait_send()
        relayed(p).wait_send()
        for s in range(4):
            across(p, s).wait_send()
    for k in range(2):
        for o in range(3):
            weight(k, o).wait_send()
    for part in range(2):
        for j in range(4):
            @pl.when(z != j)
            def _():
                reduce_copy(part, j).wait_send()


def fused(inputs, cotangent, w_in, w_out, prec_in, prec_out):
    seq, local = inputs.shape
    depth, hid = w_in.shape
    width = 4 * depth
    images = 8 * local // width
    vmem, hbm = pl.BlockSpec(memory_space=pltpu.VMEM), pl.BlockSpec(memory_space=pl.ANY)
    out = [
        jax.ShapeDtypeStruct(prec_in.shape, F32),
        jax.ShapeDtypeStruct(prec_out.shape, F32),
        jax.ShapeDtypeStruct(prec_in.shape, F32),
        jax.ShapeDtypeStruct(prec_out.shape, F32),
    ]
    dma = pltpu.SemaphoreType.DMA
    return pl.pallas_call(
        kernel,
        out_shape=out,
        in_specs=[hbm, hbm] + [vmem] * 5,
        out_specs=[vmem] * 4,
        scratch_shapes=[
            pltpu.VMEM((images, seq, width), BF16),
            pltpu.VMEM((images, seq, width), BF16),
            pltpu.VMEM((width, hid), BF16),
            pltpu.VMEM((width, hid), BF16),
            pltpu.VMEM((hid, width), BF16),
            pltpu.VMEM((hid, width), BF16),
            pltpu.VMEM((images, hid, seq), BF16),
            pltpu.VMEM((images, hid, seq), F32),
            pltpu.VMEM((images, hid, seq), F32),
            pltpu.VMEM((images, hid, seq), BF16),
            pltpu.VMEM((2, hid, width), F32),
            pltpu.VMEM((2, 2, width, hid), F32),
            pltpu.VMEM((2, 2, width, hid), BF16),
            pltpu.VMEM((2, 3, 2, depth, hid), BF16),
            dma((4,)), dma((8, 3)), dma((8, 3)), dma((8, 4)), dma((8, 4)),
            dma((2, 3)), dma((2, 3)), dma((2, 4)), dma((2, 3)),
        ],
        compiler_params=pltpu.CompilerParams(
            collective_id=0, has_side_effects=True, vmem_limit_bytes=60 * 1024 * 1024
        ),
    )(inputs, cotangent, w_in, w_out.T, w_out, prec_in, prec_out)


def solution(mesh):
    placed = (
        P(None, ("dp", "mp")),
        P(None, ("dp", "mp")),
        P("dp", "mp"),
        P("mp", "dp"),
        P("dp", "mp"),
        P("mp", "dp"),
    )
    body = fused if dict(mesh.shape) == {"dp": 4, "mp": 8} else per_device
    return jax.shard_map(
        body,
        mesh=mesh,
        in_specs=placed,
        out_specs=(P("dp", "mp"), P("mp", "dp"), P("dp", "mp"), P("mp", "dp")),
        check_vma=False,
    )
```

```python
import functools
import jax
import jax.numpy as jnp
from jax import lax
from jax.experimental import pallas as pl
from jax.experimental.pallas import tpu as pltpu
from jax.sharding import PartitionSpec as P


def gelu_tanh(v):
    return jax.nn.gelu(v, approximate=True)


def per_device(inputs, cotangent, w_in, w_out, prec_in, prec_out):
    SEQ = inputs.shape[0]
    D = w_in.shape[0] * lax.axis_size("dp")
    w_in_full, w_out_full = (
        lax.all_gather(w_in, "dp", axis=0, tiled=True),
        lax.all_gather(w_out, "dp", axis=1, tiled=True),
    )
    whole = lax.all_gather(inputs, "mp", axis=1, tiled=True)
    rows3 = whole.reshape(SEQ, -1, D)
    images = rows3.shape[1]
    pre = jnp.einsum("snd,dh->snh", rows3, w_in_full, preferred_element_type=jnp.float32)
    act = gelu_tanh(pre).astype(jnp.bfloat16)
    cot_whole = lax.all_gather(cotangent, "mp", axis=1, tiled=True)
    cot3 = cot_whole.reshape(SEQ, images, D)
    back = jnp.einsum("snd,hd->snh", cot3, w_out_full, preferred_element_type=jnp.float32)
    per_out = jnp.einsum("snh,snd->nhd", act, cot3, preferred_element_type=jnp.float32)
    sum_out = jnp.sum(per_out, 0)
    sq_out = jnp.sum(per_out * per_out, 0)
    delta = jax.vjp(gelu_tanh, pre)[1](back)[0].astype(jnp.bfloat16)
    rows_again = lax.all_gather(inputs, "mp", axis=1, tiled=True).reshape(SEQ, images, D)
    per_in = jnp.einsum("snd,snh->ndh", rows_again, delta, preferred_element_type=jnp.float32)
    sum_in = jnp.sum(per_in, 0)
    sq_in = jnp.sum(per_in * per_in, 0)
    sum_in, sq_in = (
        lax.psum_scatter(sum_in, "dp", scatter_dimension=0, tiled=True),
        lax.psum_scatter(sq_in, "dp", scatter_dimension=0, tiled=True),
    )
    sum_out, sq_out = (
        lax.psum_scatter(sum_out, "dp", scatter_dimension=1, tiled=True),
        lax.psum_scatter(sq_out, "dp", scatter_dimension=1, tiled=True),
    )
    scale = 1.0 / (images * lax.axis_size("dp"))
    new_prec_in = 0.6 * prec_in + 0.4 * sq_in * scale
    new_prec_out = 0.6 * prec_out + 0.4 * sq_out * scale
    w_in_own = w_in.astype(jnp.float32)
    w_out_own = w_out.astype(jnp.float32)
    new_w_in = w_in_own - 1.0 * (sum_in * scale + 0.1 * w_in_own) / (new_prec_in + 0.1)
    new_w_out = w_out_own - 1.0 * (sum_out * scale + 0.1 * w_out_own) / (new_prec_out + 0.1)
    return (new_prec_in, new_prec_out, new_w_in, new_w_out)


F32, BF16 = jnp.float32, jnp.bfloat16
NT = (((1,), (1,)), ((), ()))
MESH = pl.DeviceIdType.MESH


def dot(a, b):
    return jnp.dot(a, b, preferred_element_type=F32)


def dot_nt(a, b):
    return lax.dot_general(a, b, NT, preferred_element_type=F32)


def kernel(
    x_hbm, c_hbm, win_ref, wout_t_ref, sums_in, sums_out,
    xg, cg, wg_in, wg_out, w_in_t, w_out_f, act, slope, back, delta,
    acc, own, stage, recv, passing, joined,
    loc, ici_s, ici_r, d2d_s, d2d_r, w_s, w_r, rs_s, rs_r, pass_r,
):
    z, m = lax.axis_index("dp"), lax.axis_index("mp")
    core, q = lax.rem(m, 2), m // 2
    xx, yy = lax.rem(q, 2), q // 2
    chips = [yy * 2 + xx, yy * 2 + 1 - xx, (1 - yy) * 2 + xx, (1 - yy) * 2 + 1 - xx]
    same = [2 * chip + core for chip in chips]
    other = [2 * chip + 1 - core for chip in chips]
    xn, yn, partner_id = same[1], same[2], other[0]
    depth = win_ref.shape[0]
    width = 4 * depth
    lo = -(-depth // 128) * 128
    hi = 3 * depth // 128 * 128
    ranges = ((0, lo), (hi, width), (lo, hi))
    images = xg.shape[0]

    def view(p, mm):
        if p < 2:
            return xg.at[2 * mm + p]
        left, right = ranges[(p - 2) // 2]
        return cg.at[2 * mm + (p - 2) % 2, :, pl.ds(left, right - left)]

    def remote(p, mm, to, ssem, rsem):
        return pltpu.make_async_remote_copy(
            src_ref=view(p, mm), dst_ref=view(p, mm), send_sem=ssem, recv_sem=rsem,
            device_id=(z, to), device_id_type=MESH,
        )

    def to_x(p):
        return remote(p, m, xn, ici_s.at[p, 0], ici_r.at[p, 0])

    def to_y(p):
        return remote(p, m, yn, ici_s.at[p, 1], ici_r.at[p, 1])

    def relayed(p):
        first = p % 2 == 0
        return remote(p, same[1 if first else 2], yn if first else xn, ici_s.at[p, 2], ici_r.at[p, 2])

    def across(p, s):
        return remote(p, same[s], partner_id, d2d_s.at[p, s], d2d_r.at[p, s])

    def arrived(p, s):
        remote(p, same[s], xn, ici_s.at[p, 0], ici_r.at[p, s - 1]).wait_recv()

    def from_partner(pieces, s):
        for p in pieces:
            remote(p, other[s], partner_id, d2d_s.at[p, s], d2d_r.at[p, s]).wait_recv()

    def own_sends(even, odd):
        for a, b in ((even, odd),):
            for p in a:
                to_x(p).start()
            for p in b:
                to_y(p).start()
            for p in b:
                to_x(p).start()
            for p in a:
                to_y(p).start()

    def relay(even, odd):
        for p in even:
            arrived(p, 1)
            relayed(p).start()
        for p in odd:
            arrived(p, 2)
            relayed(p).start()
        for p in even:
            across(p, 1).start()
        for p in odd:
            across(p, 2).start()

    def second(even, odd):
        for p in odd:
            arrived(p, 1)
            across(p, 1).start()
        for p in even:
            arrived(p, 2)
            across(p, 2).start()

    def third(even, odd):
        for p in even + odd:
            arrived(p, 3)
            across(p, 3).start()

    x_even, x_odd = [0], [1]
    a_even, a_odd = [2, 4], [3, 5]
    b_even, b_odd = [6], [7]

    locals_ = []
    for i in range(2):
        cols = pl.ds(i * width, width)
        locals_.append(pltpu.make_async_copy(x_hbm.at[:, cols], xg.at[2 * m + i], loc.at[i]))
    for i in range(2):
        cols = pl.ds(i * width, width)
        locals_.append(pltpu.make_async_copy(c_hbm.at[:, cols], cg.at[2 * m + i], loc.at[2 + i]))
    for copy in locals_:
        copy.start()

    barrier = pltpu.get_barrier_semaphore()
    zs = [lax.rem(z + o, 4) for o in (1, 2, 3)]
    peers = [(z, xn), (z, yn), (z, partner_id)] + [(there, m) for there in zs]
    for peer in peers:
        pl.semaphore_signal(barrier, inc=1, device_id=peer, device_id_type=MESH)
    pl.semaphore_wait(barrier, len(peers))

    locals_[0].wait()
    locals_[1].wait()
    own_sends(x_even, x_odd)
    for p in x_even + x_odd:
        across(p, 0).start()

    rows = pl.ds(pl.multiple_of(z * depth, 16), depth)

    def weight(k, o):
        src, dst = ((win_ref, wg_in), (wout_t_ref, wg_out))[k]
        return pltpu.make_async_remote_copy(
            src_ref=src, dst_ref=dst.at[rows], send_sem=w_s.at[k, o], recv_sem=w_r.at[k, o],
            device_id=(zs[o], m), device_id_type=MESH,
        )

    for k in range(2):
        for o in range(3):
            weight(k, o).start()
    locals_[2].wait()
    locals_[3].wait()
    for p in a_even + a_odd + b_even + b_odd:
        across(p, 0).start()
    wg_in[rows, :] = win_ref[...]
    wg_out[rows, :] = wout_t_ref[...]
    acc[...] = jnp.zeros_like(acc)

    def forward(chip):
        def one(j, carry):
            n = 4 * chip + j
            pre = dot_nt(w_in_t[...], xg[n])
            square = pre * pre
            t = jnp.tanh(0.7978845608028654 * pre * (1.0 + 0.044715 * square))
            half = 0.5 * (1.0 + t)
            act[n] = (pre * half).astype(BF16)
            slope[n] = half + 0.5 * pre * (1.0 - t * t) * (0.7978845608028654 * (1.0 + 0.134145 * square))
            return carry
        lax.fori_loop(0, 4, one, 0)

    def accumulate(lhs, rhs, first, count, span):
        cols = slice(*span)
        gs = [dot(lhs[first + j], rhs[first + j, :, cols]) for j in range(count)]
        total, squares = gs[0], gs[0] * gs[0]
        for g in gs[1:]:
            total, squares = total + g, squares + g * g
        acc[0, :, cols] += total
        acc[1, :, cols] += squares

    def chunk_a(chip):
        def pair(h, carry):
            first = 4 * chip + 2 * h
            for j in range(2):
                n = first + j
                back[n] = dot_nt(w_out_f[:, 0:lo], cg[n, :, 0:lo]) + dot_nt(w_out_f[:, hi:width], cg[n, :, hi:width])
            for span in ranges[:2]:
                accumulate(act, cg, first, 2, span)
            return carry
        lax.fori_loop(0, 2, pair, 0)

    def chunk_b(chip):
        def pair(h, carry):
            first = 4 * chip + 2 * h
            for j in range(2):
                n = first + j
                whole = back[n] + dot_nt(w_out_f[:, lo:hi], cg[n, :, lo:hi])
                delta[n] = (whole * slope[n]).astype(BF16)
            accumulate(act, cg, first, 2, ranges[2])
            return carry
        lax.fori_loop(0, 2, pair, 0)

    def settle(part, span):
        cols = slice(*span)
        for a in range(2):
            turned = acc[a, :, cols].T
            own[part, a, cols, :] = turned
            stage[part, a, cols, :] = turned.astype(BF16)
            if part == 0:
                acc[a, :, cols] = jnp.zeros_like(acc[a, :, cols])

    def block(part, j):
        return stage.at[part, :, pl.ds(j * depth, depth), :]

    def place(j):
        inner = j in (1, 2)
        return (1 - j, 3, 2, 1 - int(inner)) if j < 2 else (5 - j, 0, 1, 1 - int(inner))

    def near_copy(part, j):
        return pltpu.make_async_remote_copy(
            src_ref=block(part, j), dst_ref=recv.at[part, 0],
            send_sem=rs_s.at[part, j], recv_sem=rs_r.at[part, 0],
            device_id=(j, m), device_id_type=MESH,
        )

    def pass_copy(part, j):
        _, _, far_inner, kind = place(j)
        return pltpu.make_async_remote_copy(
            src_ref=block(part, j), dst_ref=passing.at[part, kind],
            send_sem=rs_s.at[part, j], recv_sem=pass_r.at[part, kind],
            device_id=(far_inner, m), device_id_type=MESH,
        )

    def joined_copy(part, j):
        kind = place(j)[3]
        return pltpu.make_async_remote_copy(
            src_ref=joined.at[part, kind], dst_ref=recv.at[part, 1],
            send_sem=rs_s.at[part, j], recv_sem=rs_r.at[part, 1],
            device_id=(j, m), device_id_type=MESH,
        )

    def give(part, targets):
        for j in targets:
            mate, far_end, _, _ = place(j)

            @pl.when(z == mate)
            def _():
                near_copy(part, j).start()

            @pl.when(z == far_end)
            def _():
                pass_copy(part, j).start()

    def combine(part, targets):
        for j in targets:
            _, _, far_inner, kind = place(j)

            @pl.when(z == far_inner)
            def _():
                pass_copy(part, j).wait_recv()
                for a in range(2):
                    mine = own[part, a, j * depth:(j + 1) * depth, :]
                    joined[part, kind, a] = (mine + passing[part, kind, a].astype(F32)).astype(BF16)
                joined_copy(part, j).start()

    relay(x_even, x_odd)
    own_sends(a_even, a_odd)
    for o in range(3):
        weight(0, o).wait_recv()
    w_in_t[...] = wg_in[...].astype(F32).T.astype(BF16)
    from_partner([0, 1], 0)
    forward(chips[0])
    second(x_even, x_odd)
    from_partner([0, 1], 1)
    forward(chips[1])
    from_partner([0, 1], 2)
    forward(chips[2])
    third(x_even, x_odd)
    from_partner([0, 1], 3)
    forward(chips[3])

    for o in range(3):
        weight(1, o).wait_recv()
    w_out_f[...] = wg_out[...].astype(F32).T.astype(BF16)
    pieces = a_even + a_odd
    relay(a_even, a_odd)
    own_sends(b_even, b_odd)
    from_partner(pieces, 0)
    chunk_a(chips[0])
    second(a_even, a_odd)
    from_partner(pieces, 1)
    chunk_a(chips[1])
    from_partner(pieces, 2)
    chunk_a(chips[2])
    third(a_even, a_odd)
    relay(b_even, b_odd)
    from_partner(pieces, 3)
    chunk_a(chips[3])
    settle(0, ranges[0])
    give(0, [0])
    settle(0, ranges[1])
    give(0, [3])

    pieces = b_even + b_odd
    from_partner(pieces, 0)
    chunk_b(chips[0])
    second(b_even, b_odd)
    from_partner(pieces, 1)
    chunk_b(chips[1])
    from_partner(pieces, 2)
    chunk_b(chips[2])
    third(b_even, b_odd)
    from_partner(pieces, 3)
    chunk_b(chips[3])
    settle(0, ranges[2])
    give(0, [1, 2])
    combine(0, [0, 3])

    for span, targets in zip(ranges, ([0], [3], [1, 2])):
        def four(k, carry, span=span):
            accumulate(delta, xg, 4 * k, 4, span)
            return carry
        lax.fori_loop(0, images // 4, four, 0)
        settle(1, span)
        give(1, targets)
        if span == ranges[0]:
            combine(0, [1, 2])
    combine(1, [0, 3, 1, 2])

    def collected(part, sums):
        near_copy(part, 0).wait_recv()
        joined_copy(part, 0).wait_recv()
        for a in range(2):
            total = own[part, a, rows, :]
            for t in range(2):
                total = total + recv[part, t, a].astype(F32)
            sums[a] = total

    collected(0, sums_out)
    collected(1, sums_in)

    for p in range(8):
        to_x(p).wait_send()
        to_y(p).wait_send()
        relayed(p).wait_send()
        for s in range(4):
            across(p, s).wait_send()
    for k in range(2):
        for o in range(3):
            weight(k, o).wait_send()
    for part in range(2):
        for j in range(4):
            @pl.when(z != j)
            def _():
                near_copy(part, j).wait_send()


def fused(inputs, cotangent, w_in, w_out, prec_in, prec_out):
    seq, local = inputs.shape
    depth, hid = w_in.shape
    width = 4 * depth
    images = 8 * local // width
    vmem, hbm = pl.BlockSpec(memory_space=pltpu.VMEM), pl.BlockSpec(memory_space=pl.ANY)
    dma = pltpu.SemaphoreType.DMA
    sums_in, sums_out = pl.pallas_call(
        kernel,
        out_shape=[jax.ShapeDtypeStruct((2, depth, hid), F32)] * 2,
        in_specs=[hbm, hbm] + [vmem] * 2,
        out_specs=[vmem] * 2,
        scratch_shapes=[
            pltpu.VMEM((images, seq, width), BF16),
            pltpu.VMEM((images, seq, width), BF16),
            pltpu.VMEM((width, hid), BF16),
            pltpu.VMEM((width, hid), BF16),
            pltpu.VMEM((hid, width), BF16),
            pltpu.VMEM((hid, width), BF16),
            pltpu.VMEM((images, hid, seq), BF16),
            pltpu.VMEM((images, hid, seq), F32),
            pltpu.VMEM((images, hid, seq), F32),
            pltpu.VMEM((images, hid, seq), BF16),
            pltpu.VMEM((2, hid, width), F32),
            pltpu.VMEM((2, 2, width, hid), F32),
            pltpu.VMEM((2, 2, width, hid), BF16),
            pltpu.VMEM((2, 2, 2, depth, hid), BF16),
            pltpu.VMEM((2, 2, 2, depth, hid), BF16),
            pltpu.VMEM((2, 2, 2, depth, hid), BF16),
            dma((4,)), dma((8, 3)), dma((8, 3)), dma((8, 4)), dma((8, 4)),
            dma((2, 3)), dma((2, 3)), dma((2, 4)), dma((2, 2)), dma((2, 2)),
        ],
        compiler_params=pltpu.CompilerParams(
            collective_id=0, has_side_effects=True, vmem_limit_bytes=60 * 1024 * 1024
        ),
    )(inputs, cotangent, w_in, w_out.T)

    scale = 1.0 / (images * 4)

    def updated(sums, prec, w):
        new_prec = 0.6 * prec + 0.4 * sums[1] * scale
        mean = w.astype(F32)
        return new_prec, mean - 1.0 * (sums[0] * scale + 0.1 * mean) / (new_prec + 0.1)

    new_prec_in, new_w_in = updated(sums_in, prec_in, w_in)
    new_prec_out, new_w_out = updated(sums_out, prec_out.T, w_out.T)
    return new_prec_in, new_prec_out.T, new_w_in, new_w_out.T


def solution(mesh):
    placed = (
        P(None, ("dp", "mp")),
        P(None, ("dp", "mp")),
        P("dp", "mp"),
        P("mp", "dp"),
        P("dp", "mp"),
        P("mp", "dp"),
    )
    body = fused if dict(mesh.shape) == {"dp": 4, "mp": 8} else per_device
    return jax.shard_map(
        body,
        mesh=mesh,
        in_specs=placed,
        out_specs=(P("dp", "mp"), P("mp", "dp"), P("dp", "mp"), P("mp", "dp")),
        check_vma=False,
    )
```
